32 devices in a mesh: groups: 2 (over x), dp: 16 (over z, y, core).
Axes of the slice: x: 2, y: 2, z: 4, core: 2. Of those that a mesh axis runs over, the one named last changes fastest.
Arguments:
- batch_counts: int32 [32], P(('groups', 'dp')), parts along dimension 0, may hold values from 1 to 4, 32 in all
- attn_out: bfloat16 [128, 7168], P(('groups', 'dp')), parts along dimension 0, may hold values from -6 to 6
- residual_in: bfloat16 [128, 7168], P(('groups', 'dp')), parts along dimension 0, may hold values from -64 to 64
- norm_gain: float32 [7168], replicated, may hold values from 0.5 to 1.5
- w_gate_up: bfloat16 [2, 18432, 7168], P(None, 'dp'), may hold values from -0.0625 to 0.0625
- w_down: bfloat16 [18432, 7168], P(None, 'dp'), may hold values from -0.046875 to 0.046875
- next_gain: float32 [7168], replicated, may hold values from 0.5 to 1.5
Outputs:
- hidden_out: bfloat16 [128, 7168], P(('groups', 'dp')), parts along dimension 0
- normed_out: bfloat16 [128, 7168], P(('groups', 'dp')), parts along dimension 0
The draws below stay inside these ranges and needn't reach their ends.
There are 2 independent parts, one for each index of `groups`. The reference program is written for one: setup_inputs(seed, part) draws one part's arguments, and reference() takes and returns one part's arrays. A program takes and returns all parts, laid end to end along the dimension named above; an argument that names none is the same for every part. Nothing has to cross between parts.
Inputs may be any that keep to these rules, and one draw needn't show every extreme that they name: Rank r's occupied rows are its first batch_counts[r] slots; the counts sum to exactly 32, and some rank holds 4.
All inputs are finite; a program needn't handle non-finite values. No bound on the sum of `batch_counts` on one device may be relied on, other than what follows from the above.
Results may differ from the reference program's by a relative error of at most 0.0045.
Values may be sent and summed in bfloat16 or wider, within the bound.
A program may use at most 128 MiB of HBM per device.

```python
import math
import jax
import jax.numpy as jnp
import numpy as np
from jax import lax

D = 7168
FF = 18432
SLOTS = 4
ROWS = 64
TOKENS = 32
N_DP = 16


def draw_residual_in(key, part):
    sample = jnp.clip(jax.random.normal(jax.random.fold_in(key, 37), (ROWS, D), jnp.float32), -5.0, 5.0)
    row_scale = jnp.exp(jax.random.uniform(jax.random.fold_in(key, 41), (ROWS, 1), jnp.float32, math.log(0.3), math.log(3.0)))
    col_scale = jnp.exp(jax.random.uniform(jax.random.fold_in(key, 43), (1, D), jnp.float32, math.log(0.3), math.log(3.0)))
    return (sample * row_scale * col_scale).astype(jnp.bfloat16)


def block_scale(key, extent, pieces, smallest, largest):
    def one(axis_at, parts):
        draws = jax.random.uniform(jax.random.fold_in(jax.random.fold_in(key, 6), axis_at), (parts,), jnp.float32, smallest / len(pieces), largest / len(pieces))
        return jnp.repeat(jnp.exp(draws), extent[axis_at] // parts).reshape((-1,) + (1,) * (len(extent) - axis_at - 1))

    level = one(*pieces[0])
    for cut in pieces[1:]:
        level = level * one(*cut)
    return level


def profile(count, total, bound, skew):
    loads = [(1 << 20) // math.isqrt(grade ** skew) + 1 for grade in range(2, count + 1)]
    rest, holding = total - bound - (count - 1), [1] * (count - 1)
    while rest > 0:
        candidates = [i for i in range(count - 1) if holding[i] < bound]
        pool, left = sum([loads[i] for i in candidates]), rest
        for i in candidates:
            more = min(bound - holding[i], max(1, left * loads[i] // pool), rest)
            holding[i] = holding[i] + more
            rest = rest - more
    return np.array([bound] + holding)


def ragged_sizes(stream_key, amount, total, reach, lean):
    if amount == 2:
        one = jax.random.randint(stream_key, (), max(1, total - reach), min(reach, total - 1) + 1)
        return jnp.stack([one, total - one])
    tallies = jnp.asarray(profile(amount, total, reach, lean), jnp.int32)
    twos = (amount - 1) // 2
    source_of, sink = tallies[1:1 + 2 * twos:2], tallies[2:2 + 2 * twos:2]
    margin = jnp.minimum(source_of - 1, reach - sink)
    passed = jax.random.randint(jax.random.fold_in(stream_key, 1), (twos,), 0, 1 << 20) % (margin + 1)
    tallies = tallies.at[1:1 + 2 * twos:2].set(source_of - passed).at[2:2 + 2 * twos:2].set(sink + passed)
    return tallies[jax.random.permutation(jax.random.fold_in(stream_key, 2), amount)]


def noise(stream_key, shape, scale, most, split=(), kind=jnp.bfloat16):
    gain = block_scale(stream_key, shape, split, -0.22, 0.18) if split else 1.0
    entries = jax.random.normal(stream_key, shape, jnp.float32) * scale * gain
    return jnp.minimum(jnp.maximum(entries, -most), most).astype(kind)


def setup_inputs(seed: int = 0, part: int = 0) -> dict:
    arg_keys = jax.random.split(jax.random.key(seed), 8)
    part_splits = jax.random.split(jax.random.fold_in(arg_keys[7], part), 8)
    return {
        "batch_counts": ragged_sizes(part_splits[0], N_DP, TOKENS, SLOTS, 2).astype(jnp.int32),
        "attn_out": noise(part_splits[1], (ROWS, D), 1.0, 6.0, ((0, 16),)),
        "residual_in": draw_residual_in(jax.random.fold_in(jax.random.fold_in(arg_keys[7], part), 71), part),
        "norm_gain": jnp.clip(1.0 + 0.1 * jax.random.normal(arg_keys[3], (D,), jnp.float32), 0.5, 1.5),
        "w_gate_up": noise(arg_keys[4], (2, FF, D), D ** -0.5, 0.0625, ((1, 16),)),
        "w_down": noise(arg_keys[5], (FF, D), FF ** -0.5, 0.046875, ((1, 16),)),
        "next_gain": jnp.clip(1.0 + 0.1 * jax.random.normal(arg_keys[6], (D,), jnp.float32), 0.5, 1.5),
    }


EPSILON = 1e-06

def normalize(values, weight_gain):
    mean_square = lax.optimization_barrier(jnp.mean(values * values, axis=-1, keepdims=True))
    return values * lax.rsqrt(mean_square + EPSILON) * weight_gain

def reference(batch_counts, attn_out, residual_in, norm_gain, w_gate_up, w_down, next_gain):
    slot_index = jnp.arange(ROWS, dtype=jnp.int32)
    occupied = slot_index % SLOTS < jnp.repeat(batch_counts.astype(jnp.int32), SLOTS)
    summed = residual_in.astype(jnp.float32) + attn_out.astype(jnp.float32)
    normed_in = normalize(summed, norm_gain).astype(jnp.bfloat16)
    picked = jnp.nonzero(occupied, size=TOKENS)[0].astype(jnp.int32)
    picked_rows = normed_in[picked]
    gate_part = jnp.dot(picked_rows, w_gate_up[0].T, preferred_element_type=jnp.float32)
    up_part = jnp.dot(picked_rows, w_gate_up[1].T, preferred_element_type=jnp.float32)
    activated = (jax.nn.silu(gate_part) * up_part).astype(jnp.bfloat16)
    mlp_rows = jnp.dot(activated, w_down, preferred_element_type=jnp.float32).astype(jnp.bfloat16)
    mlp_out = jnp.zeros((ROWS, mlp_rows.shape[1]), jnp.bfloat16).at[picked].set(mlp_rows)
    updated = summed + mlp_out.astype(jnp.float32)
    hidden_out = jnp.where(occupied[:, None], updated, 0.0).astype(jnp.bfloat16)
    normed_out = jnp.where(occupied[:, None], normalize(updated, next_gain), 0.0).astype(jnp.bfloat16)
    return (hidden_out, normed_out)
```

```python
import functools

import jax
import jax.numpy as jnp
from jax import lax
from jax.experimental import pallas as pl
from jax.experimental.pallas import tpu as pltpu
from jax.sharding import PartitionSpec as P

EPSILON = 1e-06


def normalize(values, weight_gain):
    mean_square = jnp.mean(values * values, axis=-1, keepdims=True)
    return values * lax.rsqrt(mean_square + EPSILON) * weight_gain


def mlp_hidden(picked_rows, w_gate_up):
    both_parts = jnp.einsum(
        "rd,gfd->grf", picked_rows, w_gate_up, preferred_element_type=jnp.float32
    )
    return (jax.nn.silu(both_parts[0]) * both_parts[1]).astype(jnp.bfloat16)


def plain_layer(batch_counts, attn_out, residual_in, norm_gain, w_gate_up, w_down, next_gain):
    slot_count = attn_out.shape[0]
    occupied = lax.broadcasted_iota(jnp.int32, (slot_count, 1), 0) < batch_counts[0]
    summed = residual_in.astype(jnp.float32) + attn_out.astype(jnp.float32)
    normed_in = normalize(summed, norm_gain).astype(jnp.bfloat16)
    hidden_rows = mlp_hidden(lax.all_gather(normed_in, "dp", axis=0, tiled=True), w_gate_up)
    down_cols = jnp.dot(
        lax.all_gather(hidden_rows, "dp", axis=1, tiled=True),
        w_down,
        preferred_element_type=jnp.float32,
    )
    mlp_out = lax.all_to_all(
        down_cols.astype(jnp.bfloat16), "dp", split_axis=0, concat_axis=1, tiled=True
    )
    updated = summed + mlp_out.astype(jnp.float32)
    hidden_out = jnp.where(occupied, updated, 0.0).astype(jnp.bfloat16)
    normed_out = jnp.where(occupied, normalize(updated, next_gain), 0.0).astype(jnp.bfloat16)
    return (hidden_out, normed_out)


LANES = 128
SUBLANES = 16
CHUNKS = 3
MESH = pl.DeviceIdType.MESH
NT = (((1,), (1,)), ((), ()))


def dot(a, b):
    return jnp.dot(a, b, preferred_element_type=jnp.float32)


class Gather:
    def __init__(self, n, at, send_sem, recv_sem):
        self.n, self.far_count = n, n // 4
        self.me = lax.axis_index("dp")
        self.core, self.near, self.far = self.me % 2, (self.me // 2) % 2, self.me // 4
        self.sibling = self.index(0, self.near, 1 - self.core)
        self.across = self.index(0, 1 - self.near, self.core)
        self.at, self.send_sem, self.recv_sem = at, send_sem, recv_sem
        self.sent = []

    def index(self, back, near, core):
        far = lax.rem(self.far - back + self.far_count, self.far_count)
        return (far * 2 + near) * 2 + core

    def copy(self, block, target, slot):
        return pltpu.make_async_remote_copy(
            src_ref=self.at(block),
            dst_ref=self.at(block),
            send_sem=self.send_sem(slot),
            recv_sem=self.recv_sem(block),
            device_id={"dp": target},
            device_id_type=MESH,
        )

    def send(self, block, target):
        copy = self.copy(block, target, len(self.sent))
        copy.start()
        self.sent.append(copy)

    def await_block(self, block):
        self.copy(block, self.sibling, 0).wait_recv()

    def far_order(self):
        steps = list(range(1, self.far_count))
        return sorted(steps, key=lambda d: min(d, self.far_count - d))

    def start(self):
        for back in reversed(self.far_order()):
            self.send(self.me, self.index(back, self.near, self.core))
        self.send(self.me, self.across)
        self.send(self.me, self.sibling)

    def after_far(self):
        for back in self.far_order():
            block = self.index(back, self.near, self.core)
            self.await_block(block)
            self.send(block, self.across)
            self.send(block, self.sibling)

    def after_near(self):
        for back in [0] + self.far_order():
            block = self.index(back, 1 - self.near, self.core)
            self.await_block(block)
            self.send(block, self.sibling)

    def after_core(self):
        for near in (self.near, 1 - self.near):
            for back in [0] + self.far_order():
                self.await_block(self.index(back, near, 1 - self.core))

    def drain(self):
        for copy in self.sent:
            copy.wait_send()


def layer_kernel(
    n, live,
    counts_ref, attn_hbm, residual_hbm, gain_hbm, gate_up_hbm, down_hbm, next_gain_hbm,
    hidden_ref, normed_ref,
    attn, residual, gain, next_gain, gate_up, down,
    summed_ref, packed_ref, rows_ref, picked_ref, act_ref, wide_ref, out_ref, back_ref, flat_ref,
    small_sem, weight_sem, down_sem, row_send, row_recv, act_send, act_recv, out_send, out_recv,
):
    me = lax.axis_index("dp")
    slots, width = attn.shape
    pack = SUBLANES // slots
    quarter = width // pack
    piece = gate_up.shape[1] // CHUNKS

    barrier = pltpu.get_barrier_semaphore()
    for step in range(1, n):
        pl.semaphore_signal(
            barrier, inc=1, device_id={"dp": lax.rem(me + step, n)}, device_id_type=MESH
        )
    small = [
        pltpu.make_async_copy(source, target, small_sem.at[k])
        for k, (source, target) in enumerate(
            [(attn_hbm, attn), (residual_hbm, residual), (gain_hbm, gain), (next_gain_hbm, next_gain)]
        )
    ]
    for copy in small:
        copy.start()
    weight_copies = []
    for c in range(CHUNKS):
        for g in range(2):
            span = pl.ds(c * piece, piece)
            copy = pltpu.make_async_copy(
                gate_up_hbm.at[g, span], gate_up.at[g, span], weight_sem.at[c * 2 + g]
            )
            copy.start()
            weight_copies.append(copy)
    down_copies = []
    for c in range(4):
        span = pl.ds(c * (n // 4), n // 4)
        copy = pltpu.make_async_copy(down_hbm.at[span], down.at[span], down_sem.at[c])
        copy.start()
        down_copies.append(copy)
    for copy in small:
        copy.wait()

    count = counts_ref[0]
    summed = residual[...].astype(jnp.float32) + attn[...].astype(jnp.float32)
    summed_ref[...] = summed
    normed = normalize(summed, gain[...])
    for q in range(pack):
        packed_ref[q * slots:(q + 1) * slots, :quarter] = normed[:, q * quarter:(q + 1) * quarter]
    packed_ref[:, quarter:] = jnp.full((SUBLANES, LANES), count, jnp.int32).astype(jnp.float32)
    rows_ref[me] = packed_ref[...].astype(jnp.bfloat16)
    wide_ref[...] = jnp.zeros_like(wide_ref)

    pl.semaphore_wait(barrier, n - 1)
    rows = Gather(
        n, lambda b: rows_ref.at[b], lambda k: row_send.at[k], lambda b: row_recv.at[b]
    )
    rows.start()
    rows.after_far()
    rows.after_near()
    rows.after_core()

    total = n * SUBLANES
    counts = rows_ref[:, :, quarter:].reshape(total, LANES)
    at_row = lax.broadcasted_iota(jnp.int32, (total, total), 0)
    at_col = lax.broadcasted_iota(jnp.int32, (total, total), 1)
    one_before = (at_row % SUBLANES == 0) & (at_row // SUBLANES < at_col // SUBLANES)
    one_before = one_before.astype(jnp.float32).astype(jnp.bfloat16)
    mean_lane = jnp.full((live, LANES), 1.0 / LANES, jnp.bfloat16)
    held = lax.dot_general(mean_lane, counts, NT, preferred_element_type=jnp.float32)
    first = dot(held.astype(jnp.bfloat16), one_before)
    token = lax.broadcasted_iota(jnp.int32, (live, total), 0).astype(jnp.float32)
    place = lax.broadcasted_iota(jnp.int32, (live, total), 1)
    slot = (place % slots).astype(jnp.float32)
    chosen = (slot < held) & (first + slot == token)
    all_rows = rows_ref[:, :, :quarter].reshape(total, quarter)
    for q in range(pack):
        pick = jnp.where(chosen & (place // slots % pack == q), 1.0, 0.0).astype(jnp.bfloat16)
        picked_ref[:, q * quarter:(q + 1) * quarter] = dot(pick, all_rows).astype(jnp.bfloat16)

    acts = [
        Gather(
            n,
            lambda b, c=c: act_ref.at[b, c],
            lambda k, c=c: act_send.at[c, k],
            lambda b, c=c: act_recv.at[c, b],
        )
        for c in range(CHUNKS)
    ]

    def hidden(c):
        span = slice(c * piece, (c + 1) * piece)
        weight_copies[2 * c].wait()
        gate = lax.dot_general(
            picked_ref[...], gate_up[0, span, :], NT, preferred_element_type=jnp.float32
        )
        weight_copies[2 * c + 1].wait()
        up = lax.dot_general(
            picked_ref[...], gate_up[1, span, :], NT, preferred_element_type=jnp.float32
        )
        act_ref[me, c] = (gate / (1.0 + jnp.exp(-gate)) * up).astype(jnp.bfloat16)
        acts[c].start()

    def project(c, total_out):
        def one(s, held_out):
            return held_out + dot(act_ref[s, c], down[s, c * piece:(c + 1) * piece, :])

        return lax.fori_loop(0, n, one, total_out)

    hidden(0)
    hidden(1)
    acts[0].after_far()
    hidden(2)
    acts[0].after_near()
    acts[1].after_far()
    for copy in down_copies:
        copy.wait()
    acts[0].after_core()
    projected = project(0, jnp.zeros((live, down.shape[2]), jnp.float32))
    acts[1].after_near()
    acts[2].after_far()
    acts[1].after_core()
    projected = project(1, projected)
    acts[2].after_near()
    acts[2].after_core()
    projected = project(2, projected)

    depth = down.shape[2]
    wide_ref[:, :depth] = projected
    wide = wide_ref[...]
    half = depth % LANES
    if half:
        wide = jnp.where(me % 2 == 1, pltpu.roll(wide, half, 1), wide)
    wide = wide.astype(jnp.bfloat16)
    tall = jnp.concatenate([wide[:, q * LANES:(q + 1) * LANES] for q in range(pack)], axis=0)
    before = (at_col % SUBLANES == 0) & (at_col // SUBLANES < at_row // SUBLANES)
    start_of = dot(before.astype(jnp.float32).astype(jnp.bfloat16), counts)[:, :1]
    back_place = lax.broadcasted_iota(jnp.int32, (total, pack * live), 0)
    back_lane = lax.broadcasted_iota(jnp.int32, (total, pack * live), 1)
    back_slot = (back_place % slots).astype(jnp.float32)
    hit = (
        (back_slot < counts[:, :1].astype(jnp.float32))
        & (start_of + back_slot == (back_lane % live).astype(jnp.float32))
        & (back_place // slots % pack == back_lane // live)
    )
    out_ref[...] = (
        dot(jnp.where(hit, 1.0, 0.0).astype(jnp.bfloat16), tall)
        .astype(jnp.bfloat16)
        .reshape(n, SUBLANES, LANES)
    )

    def out_copy(source, target, k):
        return pltpu.make_async_remote_copy(
            src_ref=out_ref.at[target],
            dst_ref=back_ref.at[source],
            send_sem=out_send.at[k],
            recv_sem=out_recv.at[source],
            device_id={"dp": target},
            device_id_type=MESH,
        )

    outs = [out_copy(me, lax.rem(me + step, n), step) for step in range(1, n)]
    for copy in outs:
        copy.start()
    back_ref[me] = out_ref[me]
    rows.drain()
    for act in acts:
        act.drain()
    for step in range(1, n):
        source = lax.rem(me + step, n)
        out_copy(source, source, step).wait_recv()

    flat_ref[...] = back_ref[...].reshape(total, LANES).astype(jnp.float32)
    for s in range(n):
        for q in range(pack):
            tile = s * depth // LANES + q
            if tile * LANES < width:
                span = slice(tile * LANES, (tile + 1) * LANES)
                row = s * SUBLANES + q * slots
                summed_ref[:, span] = summed_ref[:, span] + flat_ref[row:row + slots, :]
    updated = summed_ref[...]
    occupied = lax.broadcasted_iota(jnp.int32, (slots, 1), 0) < count
    hidden_ref[...] = jnp.where(occupied, updated, 0.0).astype(jnp.bfloat16)
    normed_out = normalize(updated, next_gain[...])
    normed_ref[...] = jnp.where(occupied, normed_out, 0.0).astype(jnp.bfloat16)
    for copy in outs:
        copy.wait_send()


def fused_layer(n, batch_counts, attn_out, residual_in, norm_gain, w_gate_up, w_down, next_gain):
    slots, width = attn_out.shape
    hidden_units = w_gate_up.shape[1]
    depth = w_down.shape[1]
    live = n * slots // 2
    pack = SUBLANES // slots
    bf16, f32 = jnp.bfloat16, jnp.float32
    sems = pltpu.SemaphoreType.DMA
    anywhere = pl.BlockSpec(memory_space=pl.ANY)
    in_vmem = pl.BlockSpec(memory_space=pltpu.VMEM)
    return pl.pallas_call(
        functools.partial(layer_kernel, n, live),
        out_shape=[jax.ShapeDtypeStruct((slots, width), bf16)] * 2,
        in_specs=[pl.BlockSpec(memory_space=pltpu.SMEM)] + [anywhere] * 6,
        out_specs=[in_vmem, in_vmem],
        scratch_shapes=[
            pltpu.VMEM((slots, width), bf16),
            pltpu.VMEM((slots, width), bf16),
            pltpu.VMEM((1, width), f32),
            pltpu.VMEM((1, width), f32),
            pltpu.VMEM(w_gate_up.shape, bf16),
            pltpu.VMEM((n, hidden_units, depth), bf16),
            pltpu.VMEM((slots, width), f32),
            pltpu.VMEM((SUBLANES, width // pack + LANES), f32),
            pltpu.VMEM((n, SUBLANES, width // pack + LANES), bf16),
            pltpu.VMEM((live, width), bf16),
            pltpu.VMEM((n, CHUNKS, live, hidden_units // CHUNKS), bf16),
            pltpu.VMEM((live, pack * LANES), f32),
            pltpu.VMEM((n, SUBLANES, LANES), bf16),
            pltpu.VMEM((n, SUBLANES, LANES), bf16),
            pltpu.VMEM((n * SUBLANES, LANES), f32),
            sems((4,)),
            sems((2 * CHUNKS,)),
            sems((4,)),
            sems((n,)),
            sems((n,)),
            sems((CHUNKS, n)),
            sems((CHUNKS, n)),
            sems((n,)),
            sems((n,)),
        ],
        compiler_params=pltpu.CompilerParams(
            collective_id=0, has_side_effects=True, vmem_limit_bytes=65 * 1000 * 1000
        ),
    )(
        batch_counts,
        attn_out,
        residual_in,
        norm_gain.reshape(1, width),
        w_gate_up,
        w_down.reshape(n, hidden_units, depth),
        next_gain.reshape(1, width),
    )


def on_device(n, *arrays):
    slots, width = arrays[1].shape
    hidden_units, depth = arrays[4].shape[1], arrays[5].shape[1]
    pack = SUBLANES // slots
    fused = (
        n % 4 == 0
        and SUBLANES % slots == 0
        and width % (pack * LANES) == 0
        and hidden_units % (CHUNKS * LANES) == 0
        and n * slots // 2 * pack == LANES
        and depth % (LANES // 2) == 0
        and depth + depth % LANES <= pack * LANES
    )
    return tuple(fused_layer(n, *arrays)) if fused else plain_layer(*arrays)


def solution(mesh):
    placed = (
        P(("groups", "dp")),
        P(("groups", "dp"), None),
        P(("groups", "dp"), None),
        P(),
        P(None, "dp", None),
        P(None, "dp"),
        P(),
    )
    return jax.shard_map(
        functools.partial(on_device, mesh.shape["dp"]),
        mesh=mesh,
        in_specs=placed,
        out_specs=(P(("groups", "dp"), None), P(("groups", "dp"), None)),
        check_vma=False,
    )
```

```python
import functools

import jax
import jax.numpy as jnp
from jax import lax
from jax.experimental import pallas as pl
from jax.experimental.pallas import tpu as pltpu
from jax.sharding import PartitionSpec as P

EPSILON = 1e-06


def normalize(values, weight_gain):
    mean_square = jnp.mean(values * values, axis=-1, keepdims=True)
    return values * lax.rsqrt(mean_square + EPSILON) * weight_gain


def mlp_hidden(picked_rows, w_gate_up):
    both_parts = jnp.einsum(
        "rd,gfd->grf", picked_rows, w_gate_up, preferred_element_type=jnp.float32
    )
    return (jax.nn.silu(both_parts[0]) * both_parts[1]).astype(jnp.bfloat16)


def plain_layer(batch_counts, attn_out, residual_in, norm_gain, w_gate_up, w_down, next_gain):
    slot_count = attn_out.shape[0]
    occupied = lax.broadcasted_iota(jnp.int32, (slot_count, 1), 0) < batch_counts[0]
    summed = residual_in.astype(jnp.float32) + attn_out.astype(jnp.float32)
    normed_in = normalize(summed, norm_gain).astype(jnp.bfloat16)
    hidden_rows = mlp_hidden(lax.all_gather(normed_in, "dp", axis=0, tiled=True), w_gate_up)
    down_cols = jnp.dot(
        lax.all_gather(hidden_rows, "dp", axis=1, tiled=True),
        w_down,
        preferred_element_type=jnp.float32,
    )
    mlp_out = lax.all_to_all(
        down_cols.astype(jnp.bfloat16), "dp", split_axis=0, concat_axis=1, tiled=True
    )
    updated = summed + mlp_out.astype(jnp.float32)
    hidden_out = jnp.where(occupied, updated, 0.0).astype(jnp.bfloat16)
    normed_out = jnp.where(occupied, normalize(updated, next_gain), 0.0).astype(jnp.bfloat16)
    return (hidden_out, normed_out)


LANES = 128
SUBLANES = 16
CHUNKS = 3
MXU_DEPTH = 256
MESH = pl.DeviceIdType.MESH
NT = (((1,), (1,)), ((), ()))


def dot(a, b):
    return jnp.dot(a, b, preferred_element_type=jnp.float32)


def chunk_bounds(units):
    depths = units // MXU_DEPTH
    sizes = [MXU_DEPTH * ((depths + CHUNKS - 1 - c) // CHUNKS) for c in range(CHUNKS)]
    sizes[1] += units - sum(sizes)
    return [(sum(sizes[:c]), sizes[c]) for c in range(CHUNKS)]


class Gather:
    def __init__(self, n, at, send_sem, recv_sem):
        self.n, self.far_count = n, n // 4
        self.me = lax.axis_index("dp")
        self.core, self.near, self.far = self.me % 2, (self.me // 2) % 2, self.me // 4
        self.sibling = self.index(self.far, self.near, 1 - self.core)
        self.across = self.index(self.far, 1 - self.near, self.core)
        self.at, self.send_sem, self.recv_sem = at, send_sem, recv_sem
        self.sent = []
        self.lines = list(self.far_lines())

    def index(self, far, near, core):
        return (far * 2 + near) * 2 + core

    def copy(self, block, target, slot):
        return pltpu.make_async_remote_copy(
            src_ref=self.at(block),
            dst_ref=self.at(block),
            send_sem=self.send_sem(slot),
            recv_sem=self.recv_sem(block),
            device_id={"dp": target},
            device_id_type=MESH,
        )

    def send(self, block, target):
        copy = self.copy(block, target, len(self.sent))
        copy.start()
        self.sent.append(copy)

    def await_block(self, block):
        self.copy(block, self.sibling, 0).wait_recv()

    def far_lines(self):
        count = self.far_count
        ranked = [
            sorted((p for p in range(count) if p != here), key=lambda p: abs(p - here))
            for here in range(count)
        ]
        for k in range(count - 1):
            far = ranked[0][k]
            for here in range(1, count):
                far = jnp.where(self.far == here, ranked[here][k], far)
            yield far

    def start(self):
        for far in reversed(self.lines):
            self.send(self.me, self.index(far, self.near, self.core))
        self.send(self.me, self.across)
        self.send(self.me, self.sibling)

    def after_far(self):
        for far in self.lines:
            block = self.index(far, self.near, self.core)
            self.await_block(block)
            self.send(block, self.across)
            self.send(block, self.sibling)

    def after_near(self):
        for far in [self.far] + self.lines:
            block = self.index(far, 1 - self.near, self.core)
            self.await_block(block)
            self.send(block, self.sibling)

    def after_core(self):
        for near in (self.near, 1 - self.near):
            for far in [self.far] + self.lines:
                self.await_block(self.index(far, near, 1 - self.core))

    def drain(self):
        for copy in self.sent:
            copy.wait_send()


def layer_kernel(
    n, live,
    counts_hbm, attn_hbm, residual_hbm, gain_hbm, gate_up_hbm, down_hbm,
    updated_ref,
    counts_ref, attn, residual, gain, gate_up, down,
    summed_ref, packed_ref, rows_ref, picked_ref, act_refs, wide_ref, out_ref, back_ref, flat_ref,
    small_sem, weight_sem, down_sem, row_send, row_recv, act_send, act_recv, out_send, out_recv,
):
    me = lax.axis_index("dp")
    slots, width = attn.shape
    pack = SUBLANES // slots
    quarter = width // pack
    units = gate_up.shape[1]
    pieces = chunk_bounds(units)
    depth = down.shape[0]

    barrier = pltpu.get_barrier_semaphore()
    for step in range(1, n):
        pl.semaphore_signal(
            barrier, inc=1, device_id={"dp": lax.rem(me + step, n)}, device_id_type=MESH
        )
    small = [
        pltpu.make_async_copy(source, target, small_sem.at[k])
        for k, (source, target) in enumerate(
            [(attn_hbm, attn), (residual_hbm, residual), (gain_hbm, gain), (counts_hbm, counts_ref)]
        )
    ]
    for copy in small:
        copy.start()
    for copy in small:
        copy.wait()
    weight_copies = []
    for c in range(CHUNKS):
        for g in range(2):
            span = pl.ds(*pieces[c])
            copy = pltpu.make_async_copy(
                gate_up_hbm.at[g, span], gate_up.at[g, span], weight_sem.at[c * 2 + g]
            )
            copy.start()
            weight_copies.append(copy)
    down_copies = []
    for c in range(4):
        span = pl.ds(c * (depth // 4), depth // 4)
        copy = pltpu.make_async_copy(down_hbm.at[span], down.at[span], down_sem.at[c])
        copy.start()
        down_copies.append(copy)

    count = counts_ref[0]
    summed = residual[...].astype(jnp.float32) + attn[...].astype(jnp.float32)
    summed_ref[...] = summed
    normed = normalize(summed, gain[...])
    for q in range(pack):
        packed_ref[q * slots:(q + 1) * slots, :quarter] = normed[:, q * quarter:(q + 1) * quarter]
    packed_ref[:, quarter:] = jnp.full((SUBLANES, LANES), count, jnp.int32).astype(jnp.float32)
    rows_ref[me] = packed_ref[...].astype(jnp.bfloat16)
    wide_ref[...] = jnp.zeros_like(wide_ref)

    pl.semaphore_wait(barrier, n - 1)
    rows = Gather(
        n, lambda b: rows_ref.at[b], lambda k: row_send.at[k], lambda b: row_recv.at[b]
    )
    rows.start()
    rows.after_far()
    rows.after_near()
    rows.after_core()

    total = n * SUBLANES
    counts = rows_ref[:, :, quarter:].reshape(total, LANES)
    at_row = lax.broadcasted_iota(jnp.int32, (total, total), 0)
    at_col = lax.broadcasted_iota(jnp.int32, (total, total), 1)
    one_before = (at_row % SUBLANES == 0) & (at_row // SUBLANES < at_col // SUBLANES)
    one_before = one_before.astype(jnp.float32).astype(jnp.bfloat16)
    mean_lane = jnp.full((live, LANES), 1.0 / LANES, jnp.bfloat16)
    held = lax.dot_general(mean_lane, counts, NT, preferred_element_type=jnp.float32)
    first = dot(held.astype(jnp.bfloat16), one_before)
    token = lax.broadcasted_iota(jnp.int32, (live, total), 0).astype(jnp.float32)
    place = lax.broadcasted_iota(jnp.int32, (live, total), 1)
    slot = (place % slots).astype(jnp.float32)
    chosen = (slot < held) & (first + slot == token)
    all_rows = rows_ref[:, :, :quarter].reshape(total, quarter)
    for q in range(pack):
        pick = jnp.where(chosen & (place // slots % pack == q), 1.0, 0.0).astype(jnp.bfloat16)
        picked_ref[:, q * quarter:(q + 1) * quarter] = dot(pick, all_rows).astype(jnp.bfloat16)

    acts = [
        Gather(
            n,
            lambda b, c=c: act_refs[c].at[b],
            lambda k, c=c: act_send.at[c, k],
            lambda b, c=c: act_recv.at[c, b],
        )
        for c in range(CHUNKS)
    ]

    def hidden(c):
        first_unit, size = pieces[c]
        span = slice(first_unit, first_unit + size)
        weight_copies[2 * c].wait()
        gate = lax.dot_general(
            picked_ref[...], gate_up[0, span, :], NT, preferred_element_type=jnp.float32
        )
        weight_copies[2 * c + 1].wait()
        up = lax.dot_general(
            picked_ref[...], gate_up[1, span, :], NT, preferred_element_type=jnp.float32
        )
        act_refs[c][me] = (gate / (1.0 + jnp.exp(-gate)) * up).astype(jnp.bfloat16)
        acts[c].start()

    def project(c, total_out):
        first_unit, size = pieces[c]
        for s in range(n):
            span = slice(s * units + first_unit, s * units + first_unit + size)
            total_out += lax.dot_general(
                down[:, span], act_refs[c][s], NT, preferred_element_type=jnp.float32
            )
        return total_out

    hidden(0)
    hidden(1)
    acts[0].after_far()
    hidden(2)
    acts[0].after_near()
    acts[1].after_far()
    for copy in down_copies:
        copy.wait()
    acts[0].after_core()
    projected = project(0, jnp.zeros((depth, live), jnp.float32))
    acts[1].after_near()
    acts[2].after_far()
    acts[1].after_core()
    projected = project(1, projected)
    acts[2].after_near()
    acts[2].after_core()
    projected = project(2, projected)

    wide_ref[:, :depth] = projected.T
    wide = wide_ref[...]
    half = depth % LANES
    if half:
        wide = jnp.where(me % 2 == 1, pltpu.roll(wide, half, 1), wide)
    wide = wide.astype(jnp.bfloat16)
    tall = jnp.concatenate([wide[:, q * LANES:(q + 1) * LANES] for q in range(pack)], axis=0)
    before = (at_col % SUBLANES == 0) & (at_col // SUBLANES < at_row // SUBLANES)
    start_of = dot(before.astype(jnp.float32).astype(jnp.bfloat16), counts)[:, :1]
    back_place = lax.broadcasted_iota(jnp.int32, (total, pack * live), 0)
    back_lane = lax.broadcasted_iota(jnp.int32, (total, pack * live), 1)
    back_slot = (back_place % slots).astype(jnp.float32)
    hit = (
        (back_slot < counts[:, :1].astype(jnp.float32))
        & (start_of + back_slot == (back_lane % live).astype(jnp.float32))
        & (back_place // slots % pack == back_lane // live)
    )
    out_ref[...] = (
        dot(jnp.where(hit, 1.0, 0.0).astype(jnp.bfloat16), tall)
        .astype(jnp.bfloat16)
        .reshape(n, SUBLANES, LANES)
    )

    def out_copy(source, target, k):
        return pltpu.make_async_remote_copy(
            src_ref=out_ref.at[target],
            dst_ref=back_ref.at[source],
            send_sem=out_send.at[k],
            recv_sem=out_recv.at[source],
            device_id={"dp": target},
            device_id_type=MESH,
        )

    outs = [out_copy(me, lax.rem(me + step, n), step) for step in range(1, n)]
    for copy in outs:
        copy.start()
    back_ref[me] = out_ref[me]
    rows.drain()
    for act in acts:
        act.drain()
    for step in range(1, n):
        source = lax.rem(me + step, n)
        out_copy(source, source, step).wait_recv()

    flat_ref[...] = back_ref[...].reshape(total, LANES).astype(jnp.float32)
    for s in range(n):
        for q in range(pack):
            tile = s * depth // LANES + q
            if tile * LANES < width:
                span = slice(tile * LANES, (tile + 1) * LANES)
                row = s * SUBLANES + q * slots
                summed_ref[:, span] = summed_ref[:, span] + flat_ref[row:row + slots, :]
    occupied = lax.broadcasted_iota(jnp.int32, (slots, 1), 0) < count
    updated_ref[...] = jnp.where(occupied, summed_ref[...], 0.0)
    for copy in outs:
        copy.wait_send()


def finish_kernel(updated_ref, next_gain_ref, hidden_ref, normed_ref):
    updated = updated_ref[...]
    hidden_ref[...] = updated.astype(jnp.bfloat16)
    normed_ref[...] = normalize(updated, next_gain_ref[...]).astype(jnp.bfloat16)


def fused_layer(n, batch_counts, attn_out, residual_in, norm_gain, w_gate_up, w_down, next_gain):
    slots, width = attn_out.shape
    hidden_units = w_gate_up.shape[1]
    depth = w_down.shape[1]
    live = n * slots // 2
    pack = SUBLANES // slots
    bf16, f32 = jnp.bfloat16, jnp.float32
    sems = pltpu.SemaphoreType.DMA
    anywhere = pl.BlockSpec(memory_space=pl.ANY)
    in_vmem = pl.BlockSpec(memory_space=pltpu.VMEM)
    updated = pl.pallas_call(
        functools.partial(layer_kernel, n, live),
        out_shape=jax.ShapeDtypeStruct((slots, width), f32),
        in_specs=[anywhere] * 6,
        out_specs=in_vmem,
        scratch_shapes=[
            pltpu.SMEM((1,), jnp.int32),
            pltpu.VMEM((slots, width), bf16),
            pltpu.VMEM((slots, width), bf16),
            pltpu.VMEM((1, width), f32),
            pltpu.VMEM(w_gate_up.shape, bf16),
            pltpu.VMEM((depth, n * hidden_units), bf16),
            pltpu.VMEM((slots, width), f32),
            pltpu.VMEM((SUBLANES, width // pack + LANES), f32),
            pltpu.VMEM((n, SUBLANES, width // pack + LANES), bf16),
            pltpu.VMEM((live, width), bf16),
            [pltpu.VMEM((n, live, size), bf16) for _, size in chunk_bounds(hidden_units)],
            pltpu.VMEM((live, pack * LANES), f32),
            pltpu.VMEM((n, SUBLANES, LANES), bf16),
            pltpu.VMEM((n, SUBLANES, LANES), bf16),
            pltpu.VMEM((n * SUBLANES, LANES), f32),
            sems((4,)),
            sems((2 * CHUNKS,)),
            sems((4,)),
            sems((n,)),
            sems((n,)),
            sems((CHUNKS, n)),
            sems((CHUNKS, n)),
            sems((n,)),
            sems((n,)),
        ],
        compiler_params=pltpu.CompilerParams(
            collective_id=0, has_side_effects=True, vmem_limit_bytes=65 * 1000 * 1000
        ),
    )(
        batch_counts,
        attn_out,
        residual_in,
        norm_gain.reshape(1, width),
        w_gate_up,
        w_down.T,
    )
    return pl.pallas_call(
        finish_kernel,
        out_shape=[jax.ShapeDtypeStruct((slots, width), bf16)] * 2,
        in_specs=[in_vmem, in_vmem],
        out_specs=[in_vmem, in_vmem],
    )(updated, next_gain.reshape(1, width))


def on_device(n, *arrays):
    slots, width = arrays[1].shape
    hidden_units, depth = arrays[4].shape[1], arrays[5].shape[1]
    pack = SUBLANES // slots
    fused = (
        n % 4 == 0
        and SUBLANES % slots == 0
        and width % (pack * LANES) == 0
        and hidden_units % LANES == 0
        and hidden_units >= CHUNKS * MXU_DEPTH
        and n * slots // 2 * pack == LANES
        and depth % (LANES // 2) == 0
        and depth % (4 * SUBLANES) == 0
        and depth + depth % LANES <= pack * LANES
    )
    return tuple(fused_layer(n, *arrays)) if fused else plain_layer(*arrays)


def solution(mesh):
    placed = (
        P(("groups", "dp")),
        P(("groups", "dp"), None),
        P(("groups", "dp"), None),
        P(),
        P(None, "dp", None),
        P(None, "dp"),
        P(),
    )
    return jax.shard_map(
        functools.partial(on_device, mesh.shape["dp"]),
        mesh=mesh,
        in_specs=placed,
        out_specs=(P(("groups", "dp"), None), P(("groups", "dp"), None)),
        check_vma=False,
    )
```

```python
import functools

import jax
import jax.numpy as jnp
from jax import lax
from jax.experimental import pallas as pl
from jax.experimental.pallas import tpu as pltpu
from jax.sharding import PartitionSpec as P

EPSILON = 1e-06


def normalize(values, weight_gain):
    mean_square = jnp.mean(values * values, axis=-1, keepdims=True)
    return values * lax.rsqrt(mean_square + EPSILON) * weight_gain


def mlp_hidden(picked_rows, w_gate_up):
    both_parts = jnp.einsum(
        "rd,gfd->grf", picked_rows, w_gate_up, preferred_element_type=jnp.float32
    )
    return (jax.nn.silu(both_parts[0]) * both_parts[1]).astype(jnp.bfloat16)


def plain_layer(batch_counts, attn_out, residual_in, norm_gain, w_gate_up, w_down, next_gain):
    slot_count = attn_out.shape[0]
    occupied = lax.broadcasted_iota(jnp.int32, (slot_count, 1), 0) < batch_counts[0]
    summed = residual_in.astype(jnp.float32) + attn_out.astype(jnp.float32)
    normed_in = normalize(summed, norm_gain).astype(jnp.bfloat16)
    hidden_rows = mlp_hidden(lax.all_gather(normed_in, "dp", axis=0, tiled=True), w_gate_up)
    down_cols = jnp.dot(
        lax.all_gather(hidden_rows, "dp", axis=1, tiled=True),
        w_down,
        preferred_element_type=jnp.float32,
    )
    mlp_out = lax.all_to_all(
        down_cols.astype(jnp.bfloat16), "dp", split_axis=0, concat_axis=1, tiled=True
    )
    updated = summed + mlp_out.astype(jnp.float32)
    hidden_out = jnp.where(occupied, updated, 0.0).astype(jnp.bfloat16)
    normed_out = jnp.where(occupied, normalize(updated, next_gain), 0.0).astype(jnp.bfloat16)
    return (hidden_out, normed_out)


LANES = 128
SUBLANES = 16
MXU_DEPTH = 256
MESH = pl.DeviceIdType.MESH
NT = (((1,), (1,)), ((), ()))


def dot(a, b):
    return jnp.dot(a, b, preferred_element_type=jnp.float32)


def chunk_bounds(units):
    return [(at, min(MXU_DEPTH, units - at)) for at in range(0, units, MXU_DEPTH)]


class Gather:
    def __init__(self, n, at, send_sem, recv_sem):
        self.n, self.far_count = n, n // 4
        self.me = lax.axis_index("dp")
        self.core, self.near, self.far = self.me % 2, (self.me // 2) % 2, self.me // 4
        self.sibling = self.index(self.far, self.near, 1 - self.core)
        self.across = self.index(self.far, 1 - self.near, self.core)
        self.at, self.send_sem, self.recv_sem = at, send_sem, recv_sem
        self.sent = []
        self.lines = list(self.far_lines())

    def index(self, far, near, core):
        return (far * 2 + near) * 2 + core

    def copy(self, block, target, slot):
        return pltpu.make_async_remote_copy(
            src_ref=self.at(block),
            dst_ref=self.at(block),
            send_sem=self.send_sem(slot),
            recv_sem=self.recv_sem(block),
            device_id={"dp": target},
            device_id_type=MESH,
        )

    def send(self, block, target):
        copy = self.copy(block, target, len(self.sent))
        copy.start()
        self.sent.append(copy)

    def await_block(self, block):
        self.copy(block, self.sibling, 0).wait_recv()

    def far_lines(self):
        count = self.far_count
        ranked = [
            sorted((p for p in range(count) if p != here), key=lambda p: abs(p - here))
            for here in range(count)
        ]
        for k in range(count - 1):
            far = ranked[0][k]
            for here in range(1, count):
                far = jnp.where(self.far == here, ranked[here][k], far)
            yield far

    def start(self):
        for far in reversed(self.lines):
            self.send(self.me, self.index(far, self.near, self.core))
        self.send(self.me, self.across)
        self.send(self.me, self.sibling)

    def after_far(self):
        for far in self.lines:
            block = self.index(far, self.near, self.core)
            self.await_block(block)
            self.send(block, self.across)
            self.send(block, self.sibling)

    def after_near(self):
        for far in [self.far] + self.lines:
            block = self.index(far, 1 - self.near, self.core)
            self.await_block(block)
            self.send(block, self.sibling)

    def after_core(self):
        for near in (self.near, 1 - self.near):
            for far in [self.far] + self.lines:
                self.await_block(self.index(far, near, 1 - self.core))

    def drain(self):
        for copy in self.sent:
            copy.wait_send()


def layer_kernel(
    n, live,
    counts_hbm, attn_hbm, residual_hbm, gain_hbm, gate_up_hbm, down_hbm,
    updated_ref,
    counts_ref, attn, residual, gain, gate_up, down,
    summed_ref, packed_ref, rows_ref, picked_ref, act_refs, wide_ref, out_ref, back_ref, flat_ref,
    small_sem, weight_sem, down_sem, row_send, row_recv, act_send, act_recv, out_send, out_recv,
):
    me = lax.axis_index("dp")
    slots, width = attn.shape
    pack = SUBLANES // slots
    quarter = width // pack
    units = gate_up.shape[1]
    pieces = chunk_bounds(units)
    chunks = len(pieces)
    depth = down.shape[0]

    barrier = pltpu.get_barrier_semaphore()
    for step in range(1, n):
        pl.semaphore_signal(
            barrier, inc=1, device_id={"dp": lax.rem(me + step, n)}, device_id_type=MESH
        )
    small = [
        pltpu.make_async_copy(source, target, small_sem.at[k])
        for k, (source, target) in enumerate(
            [(attn_hbm, attn), (residual_hbm, residual), (gain_hbm, gain), (counts_hbm, counts_ref)]
        )
    ]
    for copy in small:
        copy.start()
    for copy in small:
        copy.wait()
    weight_copies = []
    for c in range(chunks):
        for g in range(2):
            span = pl.ds(*pieces[c])
            copy = pltpu.make_async_copy(
                gate_up_hbm.at[g, span], gate_up.at[g, span], weight_sem.at[c * 2 + g]
            )
            copy.start()
            weight_copies.append(copy)
    down_copies = []
    for c in range(4):
        span = pl.ds(c * (depth // 4), depth // 4)
        copy = pltpu.make_async_copy(down_hbm.at[span], down.at[span], down_sem.at[c])
        copy.start()
        down_copies.append(copy)

    count = counts_ref[0]
    summed = residual[...].astype(jnp.float32) + attn[...].astype(jnp.float32)
    summed_ref[...] = summed
    normed = normalize(summed, gain[...])
    for q in range(pack):
        packed_ref[q * slots:(q + 1) * slots, :quarter] = normed[:, q * quarter:(q + 1) * quarter]
    packed_ref[:, quarter:] = jnp.full((SUBLANES, LANES), count, jnp.int32).astype(jnp.float32)
    rows_ref[me] = packed_ref[...].astype(jnp.bfloat16)
    wide_ref[...] = jnp.zeros_like(wide_ref)

    pl.semaphore_wait(barrier, n - 1)
    rows = Gather(
        n, lambda b: rows_ref.at[b], lambda k: row_send.at[k], lambda b: row_recv.at[b]
    )
    rows.start()
    rows.after_far()
    rows.after_near()
    rows.after_core()

    total = n * SUBLANES
    counts = rows_ref[:, :, quarter:].reshape(total, LANES)
    at_row = lax.broadcasted_iota(jnp.int32, (total, total), 0)
    at_col = lax.broadcasted_iota(jnp.int32, (total, total), 1)
    one_before = (at_row % SUBLANES == 0) & (at_row // SUBLANES < at_col // SUBLANES)
    one_before = one_before.astype(jnp.float32).astype(jnp.bfloat16)
    mean_lane = jnp.full((live, LANES), 1.0 / LANES, jnp.bfloat16)
    held = lax.dot_general(mean_lane, counts, NT, preferred_element_type=jnp.float32)
    first = dot(held.astype(jnp.bfloat16), one_before)
    token = lax.broadcasted_iota(jnp.int32, (live, total), 0).astype(jnp.float32)
    place = lax.broadcasted_iota(jnp.int32, (live, total), 1)
    slot = (place % slots).astype(jnp.float32)
    chosen = (slot < held) & (first + slot == token)
    all_rows = rows_ref[:, :, :quarter].reshape(total, quarter)
    for q in range(pack):
        pick = jnp.where(chosen & (place // slots % pack == q), 1.0, 0.0).astype(jnp.bfloat16)
        picked_ref[:, q * quarter:(q + 1) * quarter] = dot(pick, all_rows).astype(jnp.bfloat16)

    acts = [
        Gather(
            n,
            lambda b, c=c: act_refs[c].at[b],
            lambda k, c=c: act_send.at[c, k],
            lambda b, c=c: act_recv.at[c, b],
        )
        for c in range(chunks)
    ]

    def hidden(c):
        first_unit, size = pieces[c]
        span = slice(first_unit, first_unit + size)
        weight_copies[2 * c].wait()
        weight_copies[2 * c + 1].wait()
        both = lax.dot_general(
            picked_ref[...],
            gate_up[:, span, :].reshape(2 * size, width),
            NT,
            preferred_element_type=jnp.float32,
        )
        gate, up = both[:, :size], both[:, size:]
        act_refs[c][me] = (gate / (1.0 + jnp.exp(-gate)) * up).astype(jnp.bfloat16)
        acts[c].start()

    def project(c):
        first_unit, size = pieces[c]
        acts[c].after_core()
        every = jnp.concatenate([act_refs[c][s] for s in range(n)], axis=1)
        weights = jnp.concatenate(
            [down[:, s * units + first_unit:s * units + first_unit + size] for s in range(n)], axis=1
        )
        part = lax.dot_general(every, weights, NT, preferred_element_type=jnp.float32)
        if c == 0:
            wide_ref[:, :depth] = part
        else:
            wide_ref[:, :depth] += part

    far_lag, near_lag, project_lag = 2, 3, 5
    for step in range(chunks + project_lag):
        if step < chunks:
            hidden(step)
        if step == chunks:
            for copy in down_copies:
                copy.wait()
        if 0 <= step - project_lag < chunks:
            project(step - project_lag)
        if 0 <= step - far_lag < chunks:
            acts[step - far_lag].after_far()
        if 0 <= step - near_lag < chunks:
            acts[step - near_lag].after_near()

    wide = wide_ref[...]
    half = depth % LANES
    if half:
        wide = jnp.where(me % 2 == 1, pltpu.roll(wide, half, 1), wide)
    wide = wide.astype(jnp.bfloat16)
    tall = jnp.concatenate([wide[:, q * LANES:(q + 1) * LANES] for q in range(pack)], axis=0)
    before = (at_col % SUBLANES == 0) & (at_col // SUBLANES < at_row // SUBLANES)
    start_of = dot(before.astype(jnp.float32).astype(jnp.bfloat16), counts)[:, :1]
    back_place = lax.broadcasted_iota(jnp.int32, (total, pack * live), 0)
    back_lane = lax.broadcasted_iota(jnp.int32, (total, pack * live), 1)
    back_slot = (back_place % slots).astype(jnp.float32)
    hit = (
        (back_slot < counts[:, :1].astype(jnp.float32))
        & (start_of + back_slot == (back_lane % live).astype(jnp.float32))
        & (back_place // slots % pack == back_lane // live)
    )
    out_ref[...] = (
        dot(jnp.where(hit, 1.0, 0.0).astype(jnp.bfloat16), tall)
        .astype(jnp.bfloat16)
        .reshape(n, SUBLANES, LANES)
    )

    def out_copy(source, target, k):
        return pltpu.make_async_remote_copy(
            src_ref=out_ref.at[target],
            dst_ref=back_ref.at[source],
            send_sem=out_send.at[k],
            recv_sem=out_recv.at[source],
            device_id={"dp": target},
            device_id_type=MESH,
        )

    outs = [out_copy(me, lax.rem(me + step, n), step) for step in range(1, n)]
    for copy in outs:
        copy.start()
    back_ref[me] = out_ref[me]
    rows.drain()
    for act in acts:
        act.drain()
    for step in range(1, n):
        source = lax.rem(me + step, n)
        out_copy(source, source, step).wait_recv()

    flat_ref[...] = back_ref[...].reshape(total, LANES).astype(jnp.float32)
    for s in range(n):
        for q in range(pack):
            tile = s * depth // LANES + q
            if tile * LANES < width:
                span = slice(tile * LANES, (tile + 1) * LANES)
                row = s * SUBLANES + q * slots
                summed_ref[:, span] = summed_ref[:, span] + flat_ref[row:row + slots, :]
    occupied = lax.broadcasted_iota(jnp.int32, (slots, 1), 0) < count
    updated_ref[...] = jnp.where(occupied, summed_ref[...], 0.0)
    for copy in outs:
        copy.wait_send()


def finish_kernel(updated_ref, next_gain_ref, hidden_ref, normed_ref):
    updated = updated_ref[...]
    hidden_ref[...] = updated.astype(jnp.bfloat16)
    normed_ref[...] = normalize(updated, next_gain_ref[...]).astype(jnp.bfloat16)


def fused_layer(n, batch_counts, attn_out, residual_in, norm_gain, w_gate_up, w_down, next_gain):
    slots, width = attn_out.shape
    hidden_units = w_gate_up.shape[1]
    depth = w_down.shape[1]
    live = n * slots // 2
    pack = SUBLANES // slots
    pieces = chunk_bounds(hidden_units)
    chunks = len(pieces)
    bf16, f32 = jnp.bfloat16, jnp.float32
    sems = pltpu.SemaphoreType.DMA
    anywhere = pl.BlockSpec(memory_space=pl.ANY)
    in_vmem = pl.BlockSpec(memory_space=pltpu.VMEM)
    updated = pl.pallas_call(
        functools.partial(layer_kernel, n, live),
        out_shape=jax.ShapeDtypeStruct((slots, width), f32),
        in_specs=[anywhere] * 6,
        out_specs=in_vmem,
        scratch_shapes=[
            pltpu.SMEM((1,), jnp.int32),
            pltpu.VMEM((slots, width), bf16),
            pltpu.VMEM((slots, width), bf16),
            pltpu.VMEM((1, width), f32),
            pltpu.VMEM(w_gate_up.shape, bf16),
            pltpu.VMEM((depth, n * hidden_units), bf16),
            pltpu.VMEM((slots, width), f32),
            pltpu.VMEM((SUBLANES, width // pack + LANES), f32),
            pltpu.VMEM((n, SUBLANES, width // pack + LANES), bf16),
            pltpu.VMEM((live, width), bf16),
            [pltpu.VMEM((n, live, size), bf16) for _, size in pieces],
            pltpu.VMEM((live, pack * LANES), f32),
            pltpu.VMEM((n, SUBLANES, LANES), bf16),
            pltpu.VMEM((n, SUBLANES, LANES), bf16),
            pltpu.VMEM((n * SUBLANES, LANES), f32),
            sems((4,)),
            sems((2 * chunks,)),
            sems((4,)),
            sems((n,)),
            sems((n,)),
            sems((chunks, n)),
            sems((chunks, n)),
            sems((n,)),
            sems((n,)),
        ],
        compiler_params=pltpu.CompilerParams(
            collective_id=0, has_side_effects=True, vmem_limit_bytes=65 * 1000 * 1000
        ),
    )(
        batch_counts,
        attn_out,
        residual_in,
        norm_gain.reshape(1, width),
        w_gate_up,
        w_down.T,
    )
    return pl.pallas_call(
        finish_kernel,
        out_shape=[jax.ShapeDtypeStruct((slots, width), bf16)] * 2,
        in_specs=[in_vmem, in_vmem],
        out_specs=[in_vmem, in_vmem],
    )(updated, next_gain.reshape(1, width))


def on_device(n, *arrays):
    slots, width = arrays[1].shape
    hidden_units, depth = arrays[4].shape[1], arrays[5].shape[1]
    pack = SUBLANES // slots
    fused = (
        n % 4 == 0
        and SUBLANES % slots == 0
        and width % (pack * LANES) == 0
        and hidden_units % LANES == 0
        and hidden_units >= 2 * MXU_DEPTH
        and n * slots // 2 * pack == LANES
        and depth % (LANES // 2) == 0
        and depth % (4 * SUBLANES) == 0
        and depth + depth % LANES <= pack * LANES
    )
    return tuple(fused_layer(n, *arrays)) if fused else plain_layer(*arrays)


def solution(mesh):
    placed = (
        P(("groups", "dp")),
        P(("groups", "dp"), None),
        P(("groups", "dp"), None),
        P(),
        P(None, "dp", None),
        P(None, "dp"),
        P(),
    )
    return jax.shard_map(
        functools.partial(on_device, mesh.shape["dp"]),
        mesh=mesh,
        in_specs=placed,
        out_specs=(P(("groups", "dp"), None), P(("groups", "dp"), None)),
        check_vma=False,
    )
```

```python
import functools

import jax
import jax.numpy as jnp
from jax import lax
from jax.experimental import pallas as pl
from jax.experimental.pallas import tpu as pltpu
from jax.sharding import PartitionSpec as P

EPSILON = 1e-06


def normalize(values, weight_gain):
    mean_square = jnp.mean(values * values, axis=-1, keepdims=True)
    return values * lax.rsqrt(mean_square + EPSILON) * weight_gain


def mlp_hidden(picked_rows, w_gate_up):
    both_parts = jnp.einsum(
        "rd,gfd->grf", picked_rows, w_gate_up, preferred_element_type=jnp.float32
    )
    return (jax.nn.silu(both_parts[0]) * both_parts[1]).astype(jnp.bfloat16)


def plain_layer(batch_counts, attn_out, residual_in, norm_gain, w_gate_up, w_down, next_gain):
    slot_count = attn_out.shape[0]
    occupied = lax.broadcasted_iota(jnp.int32, (slot_count, 1), 0) < batch_counts[0]
    summed = residual_in.astype(jnp.float32) + attn_out.astype(jnp.float32)
    normed_in = normalize(summed, norm_gain).astype(jnp.bfloat16)
    hidden_rows = mlp_hidden(lax.all_gather(normed_in, "dp", axis=0, tiled=True), w_gate_up)
    down_cols = jnp.dot(
        lax.all_gather(hidden_rows, "dp", axis=1, tiled=True),
        w_down,
        preferred_element_type=jnp.float32,
    )
    mlp_out = lax.all_to_all(
        down_cols.astype(jnp.bfloat16), "dp", split_axis=0, concat_axis=1, tiled=True
    )
    updated = summed + mlp_out.astype(jnp.float32)
    hidden_out = jnp.where(occupied, updated, 0.0).astype(jnp.bfloat16)
    normed_out = jnp.where(occupied, normalize(updated, next_gain), 0.0).astype(jnp.bfloat16)
    return (hidden_out, normed_out)


LANES = 128
SUBLANES = 16
MXU_DEPTH = 256
MESH = pl.DeviceIdType.MESH
NT = (((1,), (1,)), ((), ()))


def dot(a, b):
    return jnp.dot(a, b, preferred_element_type=jnp.float32)


def chunk_bounds(units):
    return [(at, min(MXU_DEPTH, units - at)) for at in range(0, units, MXU_DEPTH)]


class Gather:
    def __init__(self, n, at, send_sem, recv_sem):
        self.n, self.far_count = n, n // 4
        self.me = lax.axis_index("dp")
        self.core, self.near, self.far = self.me % 2, (self.me // 2) % 2, self.me // 4
        self.sibling = self.index(self.far, self.near, 1 - self.core)
        self.across = self.index(self.far, 1 - self.near, self.core)
        self.at, self.send_sem, self.recv_sem = at, send_sem, recv_sem
        self.sent = []
        self.lines = list(self.far_lines())

    def index(self, far, near, core):
        return (far * 2 + near) * 2 + core

    def copy(self, block, target, slot):
        return pltpu.make_async_remote_copy(
            src_ref=self.at(block),
            dst_ref=self.at(block),
            send_sem=self.send_sem(slot),
            recv_sem=self.recv_sem(block),
            device_id={"dp": target},
            device_id_type=MESH,
        )

    def send(self, block, target):
        copy = self.copy(block, target, len(self.sent))
        copy.start()
        self.sent.append(copy)

    def await_block(self, block):
        self.copy(block, self.sibling, 0).wait_recv()

    def far_lines(self):
        count = self.far_count
        ranked = [
            sorted((p for p in range(count) if p != here), key=lambda p: abs(p - here))
            for here in range(count)
        ]
        for k in range(count - 1):
            far = ranked[0][k]
            for here in range(1, count):
                far = jnp.where(self.far == here, ranked[here][k], far)
            yield far

    def start(self):
        for far in self.lines:
            self.send(self.me, self.index(far, self.near, self.core))
        self.send(self.me, self.across)
        self.send(self.me, self.sibling)

    def after_far(self):
        for far in self.lines:
            block = self.index(far, self.near, self.core)
            self.await_block(block)
            self.send(block, self.across)
            self.send(block, self.sibling)

    def after_near(self):
        for far in [self.far] + self.lines:
            block = self.index(far, 1 - self.near, self.core)
            self.await_block(block)
            self.send(block, self.sibling)

    def after_core(self):
        for near in (self.near, 1 - self.near):
            for far in [self.far] + self.lines:
                self.await_block(self.index(far, near, 1 - self.core))

    def drain(self):
        for copy in self.sent:
            copy.wait_send()


def layer_kernel(
    n, live,
    counts_hbm, attn_hbm, residual_hbm, gain_hbm, gate_up_hbm, down_hbm,
    updated_ref,
    counts_ref, attn, residual, gain, gate_up, down,
    summed_ref, packed_ref, rows_ref, picked_ref, act_refs, wide_ref, out_ref, back_ref, flat_ref,
    small_sem, weight_sem, down_sem, row_send, row_recv, act_send, act_recv, out_send, out_recv,
):
    me = lax.axis_index("dp")
    slots, width = attn.shape
    pack = SUBLANES // slots
    quarter = width // pack
    units = gate_up.shape[1]
    pieces = chunk_bounds(units)
    chunks = len(pieces)
    depth = down.shape[0]

    barrier = pltpu.get_barrier_semaphore()
    for step in range(1, n):
        pl.semaphore_signal(
            barrier, inc=1, device_id={"dp": lax.rem(me + step, n)}, device_id_type=MESH
        )
    small = [
        pltpu.make_async_copy(source, target, small_sem.at[k])
        for k, (source, target) in enumerate(
            [(attn_hbm, attn), (residual_hbm, residual), (gain_hbm, gain), (counts_hbm, counts_ref)]
        )
    ]
    for copy in small:
        copy.start()
    for copy in small:
        copy.wait()
    weight_copies = []
    for c in range(chunks):
        for g in range(2):
            span = pl.ds(*pieces[c])
            copy = pltpu.make_async_copy(
                gate_up_hbm.at[g, span], gate_up.at[g, span], weight_sem.at[c * 2 + g]
            )
            copy.start()
            weight_copies.append(copy)
    down_copies = []
    for c in range(4):
        span = pl.ds(c * (depth // 4), depth // 4)
        copy = pltpu.make_async_copy(down_hbm.at[span], down.at[span], down_sem.at[c])
        copy.start()
        down_copies.append(copy)

    count = counts_ref[0]
    summed = residual[...].astype(jnp.float32) + attn[...].astype(jnp.float32)
    summed_ref[...] = summed
    normed = normalize(summed, gain[...])
    for q in range(pack):
        packed_ref[q * slots:(q + 1) * slots, :quarter] = normed[:, q * quarter:(q + 1) * quarter]
    packed_ref[:, quarter:] = jnp.full((SUBLANES, LANES), count, jnp.int32).astype(jnp.float32)
    rows_ref[me] = packed_ref[...].astype(jnp.bfloat16)
    wide_ref[...] = jnp.zeros_like(wide_ref)

    pl.semaphore_wait(barrier, n - 1)
    rows = Gather(
        n, lambda b: rows_ref.at[b], lambda k: row_send.at[k], lambda b: row_recv.at[b]
    )
    rows.start()
    rows.after_far()
    rows.after_near()
    rows.after_core()

    total = n * SUBLANES
    counts = rows_ref[:, :, quarter:].reshape(total, LANES)
    at_row = lax.broadcasted_iota(jnp.int32, (total, total), 0)
    at_col = lax.broadcasted_iota(jnp.int32, (total, total), 1)
    one_before = (at_row % SUBLANES == 0) & (at_row // SUBLANES < at_col // SUBLANES)
    one_before = one_before.astype(jnp.float32).astype(jnp.bfloat16)
    mean_lane = jnp.full((live, LANES), 1.0 / LANES, jnp.bfloat16)
    held = lax.dot_general(mean_lane, counts, NT, preferred_element_type=jnp.float32)
    first = dot(held.astype(jnp.bfloat16), one_before)
    token = lax.broadcasted_iota(jnp.int32, (live, total), 0).astype(jnp.float32)
    place = lax.broadcasted_iota(jnp.int32, (live, total), 1)
    slot = (place % slots).astype(jnp.float32)
    chosen = (slot < held) & (first + slot == token)
    all_rows = rows_ref[:, :, :quarter].reshape(total, quarter)
    for q in range(pack):
        pick = jnp.where(chosen & (place // slots % pack == q), 1.0, 0.0).astype(jnp.bfloat16)
        picked_ref[:, q * quarter:(q + 1) * quarter] = dot(pick, all_rows).astype(jnp.bfloat16)

    acts = [
        Gather(
            n,
            lambda b, c=c: act_refs[c].at[b],
            lambda k, c=c: act_send.at[c, k],
            lambda b, c=c: act_recv.at[c, b],
        )
        for c in range(chunks)
    ]

    def hidden(c):
        first_unit, size = pieces[c]
        span = slice(first_unit, first_unit + size)
        weight_copies[2 * c].wait()
        weight_copies[2 * c + 1].wait()
        both = lax.dot_general(
            picked_ref[...],
            gate_up[:, span, :].reshape(2 * size, width),
            NT,
            preferred_element_type=jnp.float32,
        )
        gate, up = both[:, :size], both[:, size:]
        act_refs[c][me] = (gate / (1.0 + jnp.exp(-gate)) * up).astype(jnp.bfloat16)
        acts[c].start()

    def project(c):
        first_unit, size = pieces[c]
        acts[c].after_core()
        every = jnp.concatenate([act_refs[c][s] for s in range(n)], axis=1)
        weights = jnp.concatenate(
            [down[:, s * units + first_unit:s * units + first_unit + size] for s in range(n)], axis=1
        )
        part = lax.dot_general(every, weights, NT, preferred_element_type=jnp.float32)
        if c == 0:
            wide_ref[:, :depth] = part
        else:
            wide_ref[:, :depth] += part

    far_lag, near_lag, project_lag = 2, 3, 5
    for step in range(chunks + project_lag):
        if step < chunks:
            hidden(step)
        if step == chunks:
            for copy in down_copies:
                copy.wait()
        if 0 <= step - project_lag < chunks:
            project(step - project_lag)
        if 0 <= step - far_lag < chunks:
            acts[step - far_lag].after_far()
        if 0 <= step - near_lag < chunks:
            acts[step - near_lag].after_near()

    wide = wide_ref[...]
    half = depth % LANES
    if half:
        wide = jnp.where(me % 2 == 1, pltpu.roll(wide, half, 1), wide)
    wide = wide.astype(jnp.bfloat16)
    tall = jnp.concatenate([wide[:, q * LANES:(q + 1) * LANES] for q in range(pack)], axis=0)
    before = (at_col % SUBLANES == 0) & (at_col // SUBLANES < at_row // SUBLANES)
    start_of = dot(before.astype(jnp.float32).astype(jnp.bfloat16), counts)[:, :1]
    back_place = lax.broadcasted_iota(jnp.int32, (total, pack * live), 0)
    back_lane = lax.broadcasted_iota(jnp.int32, (total, pack * live), 1)
    back_slot = (back_place % slots).astype(jnp.float32)
    hit = (
        (back_slot < counts[:, :1].astype(jnp.float32))
        & (start_of + back_slot == (back_lane % live).astype(jnp.float32))
        & (back_place // slots % pack == back_lane // live)
    )
    out_ref[...] = (
        dot(jnp.where(hit, 1.0, 0.0).astype(jnp.bfloat16), tall)
        .astype(jnp.bfloat16)
        .reshape(n, SUBLANES, LANES)
    )

    def out_copy(source, target, k):
        return pltpu.make_async_remote_copy(
            src_ref=out_ref.at[target],
            dst_ref=back_ref.at[source],
            send_sem=out_send.at[k],
            recv_sem=out_recv.at[source],
            device_id={"dp": target},
            device_id_type=MESH,
        )

    outs = [out_copy(me, lax.rem(me + step, n), step) for step in range(1, n)]
    for copy in outs:
        copy.start()
    back_ref[me] = out_ref[me]
    rows.drain()
    for act in acts:
        act.drain()
    for step in range(1, n):
        source = lax.rem(me + step, n)
        out_copy(source, source, step).wait_recv()

    flat_ref[...] = back_ref[...].reshape(total, LANES).astype(jnp.float32)
    for s in range(n):
        for q in range(pack):
            tile = s * depth // LANES + q
            if tile * LANES < width:
                span = slice(tile * LANES, (tile + 1) * LANES)
                row = s * SUBLANES + q * slots
                summed_ref[:, span] = summed_ref[:, span] + flat_ref[row:row + slots, :]
    occupied = lax.broadcasted_iota(jnp.int32, (slots, 1), 0) < count
    updated_ref[...] = jnp.where(occupied, summed_ref[...], 0.0)
    for copy in outs:
        copy.wait_send()


def finish_kernel(updated_ref, next_gain_ref, hidden_ref, normed_ref):
    updated = updated_ref[...]
    hidden_ref[...] = updated.astype(jnp.bfloat16)
    normed_ref[...] = normalize(updated, next_gain_ref[...]).astype(jnp.bfloat16)


def fused_layer(n, batch_counts, attn_out, residual_in, norm_gain, w_gate_up, w_down, next_gain):
    slots, width = attn_out.shape
    hidden_units = w_gate_up.shape[1]
    depth = w_down.shape[1]
    live = n * slots // 2
    pack = SUBLANES // slots
    pieces = chunk_bounds(hidden_units)
    chunks = len(pieces)
    bf16, f32 = jnp.bfloat16, jnp.float32
    sems = pltpu.SemaphoreType.DMA
    anywhere = pl.BlockSpec(memory_space=pl.ANY)
    in_vmem = pl.BlockSpec(memory_space=pltpu.VMEM)
    updated = pl.pallas_call(
        functools.partial(layer_kernel, n, live),
        out_shape=jax.ShapeDtypeStruct((slots, width), f32),
        in_specs=[anywhere] * 6,
        out_specs=in_vmem,
        scratch_shapes=[
            pltpu.SMEM((1,), jnp.int32),
            pltpu.VMEM((slots, width), bf16),
            pltpu.VMEM((slots, width), bf16),
            pltpu.VMEM((1, width), f32),
            pltpu.VMEM(w_gate_up.shape, bf16),
            pltpu.VMEM((depth, n * hidden_units), bf16),
            pltpu.VMEM((slots, width), f32),
            pltpu.VMEM((SUBLANES, width // pack + LANES), f32),
            pltpu.VMEM((n, SUBLANES, width // pack + LANES), bf16),
            pltpu.VMEM((live, width), bf16),
            [pltpu.VMEM((n, live, size), bf16) for _, size in pieces],
            pltpu.VMEM((live, pack * LANES), f32),
            pltpu.VMEM((n, SUBLANES, LANES), bf16),
            pltpu.VMEM((n, SUBLANES, LANES), bf16),
            pltpu.VMEM((n * SUBLANES, LANES), f32),
            sems((4,)),
            sems((2 * chunks,)),
            sems((4,)),
            sems((n,)),
            sems((n,)),
            sems((chunks, n)),
            sems((chunks, n)),
            sems((n,)),
            sems((n,)),
        ],
        compiler_params=pltpu.CompilerParams(
            collective_id=0, has_side_effects=True, vmem_limit_bytes=65 * 1000 * 1000
        ),
    )(
        batch_counts,
        attn_out,
        residual_in,
        norm_gain.reshape(1, width),
        w_gate_up,
        w_down.T,
    )
    return pl.pallas_call(
        finish_kernel,
        out_shape=[jax.ShapeDtypeStruct((slots, width), bf16)] * 2,
        in_specs=[in_vmem, in_vmem],
        out_specs=[in_vmem, in_vmem],
    )(updated, next_gain.reshape(1, width))


def on_device(n, *arrays):
    slots, width = arrays[1].shape
    hidden_units, depth = arrays[4].shape[1], arrays[5].shape[1]
    pack = SUBLANES // slots
    fused = (
        n % 4 == 0
        and SUBLANES % slots == 0
        and width % (pack * LANES) == 0
        and hidden_units % LANES == 0
        and hidden_units >= 2 * MXU_DEPTH
        and n * slots // 2 * pack == LANES
        and depth % (LANES // 2) == 0
        and depth % (4 * SUBLANES) == 0
        and depth + depth % LANES <= pack * LANES
    )
    return tuple(fused_layer(n, *arrays)) if fused else plain_layer(*arrays)


def solution(mesh):
    placed = (
        P(("groups", "dp")),
        P(("groups", "dp"), None),
        P(("groups", "dp"), None),
        P(),
        P(None, "dp", None),
        P(None, "dp"),
        P(),
    )
    return jax.shard_map(
        functools.partial(on_device, mesh.shape["dp"]),
        mesh=mesh,
        in_specs=placed,
        out_specs=(P(("groups", "dp"), None), P(("groups", "dp"), None)),
        check_vma=False,
    )
```
